32 devices in a mesh: ep: 4 (over y, x), fsdp: 8 (over z, core).
Axes of the slice: x: 2, y: 2, z: 4, core: 2. Of those that a mesh axis runs over, the one named last changes fastest.
Arguments:
- train_gate: float32 [64, 2048, 1408], P('ep', 'fsdp'), may hold values from -0.1875 to 0.1875
- other_gate: bfloat16 [64, 2048, 1408], P('ep', 'fsdp'), may hold values from -0.0625 to 0.0625
- train_up: float32 [64, 2048, 1408], P('ep', 'fsdp'), may hold values from -0.1875 to 0.1875
- other_up: bfloat16 [64, 2048, 1408], P('ep', 'fsdp'), may hold values from -0.0625 to 0.0625
- router_weight: float32 [2048, 64], P('fsdp', 'ep'), may hold values from -0.125 to 0.125
- router_gain: float32 [2048], P('fsdp'), may hold values from 0.25 to 1.75
Outputs:
- ready_gate: bfloat16 [64, 2048, 1408], P('ep', None, 'fsdp')
- ready_up: bfloat16 [64, 2048, 1408], P('ep', None, 'fsdp')
- scale_gate: float32 [64, 1408], P('ep', 'fsdp')
- scale_up: float32 [64, 1408], P('ep', 'fsdp')
- serve_router: bfloat16 [2048, 64], replicated
The draws below stay inside these ranges and needn't reach their ends.
All inputs are finite; a program needn't handle non-finite values. Where the reference program divides by a largest or mean magnitude, that divisor is 1e-20 or more.
Results may differ from the reference program's by a relative error of at most 0.001.
Values may be sent and summed in bfloat16 or wider, within the bound.
A program may use at most 192 MiB of HBM per device.

```python
import jax
import jax.numpy as jnp

EXPERTS = 64
D_MODEL = 2048
D_EXPERT = 1408


def strengthened(array, stream_key, source, target, blocks, factor):
    owner, partner = [(jnp.arange(array.shape[axis_at]) // (array.shape[axis_at] // blocks)).reshape([-1 if axis == axis_at else 1 for axis in range(array.ndim)]) for axis_at in (source, target)]
    chosen = jax.random.permutation(stream_key, blocks)[partner]
    strong = (owner == chosen) | (owner == (partner + blocks // 2) % blocks)
    return jnp.where(strong, factor * array, array)


def steps_of(rng, shape, split, smallest, high):
    def one(axis_at, shards_of):
        heights = jax.random.uniform(jax.random.fold_in(jax.random.fold_in(rng, 6), axis_at), (shards_of,), jnp.float32, smallest / len(split), high / len(split))
        return jnp.repeat(jnp.exp(heights), shape[axis_at] // shards_of).reshape((-1,) + (1,) * (len(shape) - axis_at - 1))

    factor_of = one(*split[0])
    for cut in split[1:]:
        factor_of = factor_of * one(*cut)
    return factor_of


def normal_values(own_key, extent, spread, limit, cuts=(), held_as=jnp.bfloat16):
    entries = spread * jax.random.normal(own_key, extent, jnp.float32)
    if cuts:
        entries = entries * steps_of(own_key, extent, cuts, -0.22, 0.18)
    return jnp.clip(entries, -limit, limit).astype(held_as)


def bell_draw_with(stream_key, shape, spread, most, split, heavy, dtype=jnp.bfloat16):
    result = spread * jax.random.normal(stream_key, shape, jnp.float32)
    if split:
        result = result * steps_of(stream_key, shape, split, -0.22, 0.18)
    return jnp.clip(strengthened(result, jax.random.fold_in(stream_key, 3), *heavy), -most, most).astype(dtype)


def setup_inputs(seed: int = 0) -> dict:
    splits = jax.random.split(jax.random.key(seed), 7)
    train_gate = bell_draw_with(splits[0], (EXPERTS, D_MODEL, D_EXPERT), D_MODEL ** -0.5, 0.1875, ((0, 4), (1, 8)), (1, 2, 8, 2.0), jnp.float32)
    other_gate = normal_values(splits[1], (EXPERTS, D_MODEL, D_EXPERT), (D_MODEL * 4) ** -0.5, 0.0625, ((0, 4), (1, 8)))
    train_up = bell_draw_with(splits[2], (EXPERTS, D_MODEL, D_EXPERT), D_MODEL ** -0.5, 0.1875, ((0, 4), (1, 8)), (1, 2, 8, 2.0), jnp.float32)
    other_up = normal_values(splits[3], (EXPERTS, D_MODEL, D_EXPERT), (D_MODEL * 4) ** -0.5, 0.0625, ((0, 4), (1, 8)))
    router_weight = normal_values(splits[4], (D_MODEL, EXPERTS), D_MODEL ** -0.5, 0.125, ((0, 8), (1, 4)), jnp.float32)
    router_gain = jnp.clip(1.0 + 0.15 * jax.random.normal(splits[5], (D_MODEL,), jnp.float32), 0.25, 1.75)
    return dict(train_gate=train_gate, other_gate=other_gate, train_up=train_up, other_up=other_up, router_weight=router_weight, router_gain=router_gain)


def reference(train_gate, other_gate, train_up, other_up, router_weight, router_gain):
    latest_gate = train_gate + other_gate.astype(jnp.float32)
    latest_up = train_up + other_up.astype(jnp.float32)
    scale_gate = jnp.max(jnp.abs(latest_gate), axis=1)
    ready_gate = (latest_gate / jnp.expand_dims(scale_gate, 1)).astype(jnp.bfloat16)
    scale_up = jnp.max(jnp.abs(latest_up), axis=1)
    ready_up = (latest_up / jnp.expand_dims(scale_up, 1)).astype(jnp.bfloat16)
    serve_router = (router_weight * router_gain[:, None]).astype(jnp.bfloat16)
    return ready_gate, ready_up, scale_gate, scale_up, serve_router
```

```python
import functools

import jax
import jax.numpy as jnp
from jax import lax
from jax.experimental import pallas as pl
from jax.experimental.pallas import tpu as pltpu
from jax.sharding import PartitionSpec as P

LANES = 128
DEPTH = 3
PIECES = 8


def regroup(n, teams, tg, og, tu, ou, weight, gain, rg, ru, sg, su, router, mx, mo, nx, no, turned, blocks, own, pair, both, chips, final,
            mx_sem, mo_sem, nx_sem, no_sem, send_sem, keep_sem, recv_sem, p_send, p_recv, z_send, z_recv, f_send, f_recv,
            tops, part, row, whole, a_send, a_recv, a_keep, b_send, b_recv, b_keep):
    me, team = lax.axis_index("fsdp"), lax.axis_index("ep")
    core = lax.rem(me, 2)
    partner = me + 1 - 2 * core
    experts, rows, columns = tg.shape
    width = columns // n
    trains, others, outs = (tg, tu), (og, ou), (rg, ru)

    def loads(x, o, x_sem, o_sem, e):
        slot = lax.rem(e, 2)
        copies = []
        for t in range(2):
            copies.append(pltpu.make_async_copy(trains[t].at[e], x.at[slot, t], x_sem.at[slot, t]))
            copies.append(pltpu.make_async_copy(others[t].at[e], o.at[slot, t], o_sem.at[slot, t]))
        return copies

    def remote(src, dst, send, recv, device):
        return pltpu.make_async_remote_copy(
            src_ref=src, dst_ref=dst, send_sem=send, recv_sem=recv, device_id={"fsdp": device},
            device_id_type=pl.DeviceIdType.MESH,
        )

    def wait_bytes(ref, sem):
        pltpu.make_async_copy(ref, ref, sem).wait()

    for copy in loads(mx, mo, mx_sem, mo_sem, 0):
        copy.start()
    for copy in loads(nx, no, nx_sem, no_sem, 0):
        copy.start()
    part[...] = (weight[...] * gain[...]).astype(jnp.bfloat16)

    barrier = pltpu.get_barrier_semaphore()
    for k in range(1, n):
        pl.semaphore_signal(barrier, inc=1, device_id={"fsdp": lax.rem(me + k, n)}, device_id_type=pl.DeviceIdType.MESH)
    for k in range(1, teams):
        pl.semaphore_signal(barrier, inc=1, device_id={"ep": lax.rem(team + k, teams)}, device_id_type=pl.DeviceIdType.MESH)
    pl.semaphore_wait(barrier, n + teams - 2)

    def measure(e):
        slot = lax.rem(e, 2)

        @pl.when(e + 1 < experts)
        def _():
            for copy in loads(mx, mo, mx_sem, mo_sem, e + 1):
                copy.start()

        for copy in loads(mx, mo, mx_sem, mo_sem, e):
            copy.wait()
        for t in range(2):
            for j in range(0, columns, LANES):
                latest = mx[slot, t, :, j : j + LANES] + mo[slot, t, :, j : j + LANES].astype(jnp.float32)
                own[e, t, :, j : j + LANES] = jnp.max(jnp.abs(latest), axis=0, keepdims=True)
        remote(own.at[e, 1 - core], pair.at[e], p_send.at[e], p_recv.at[e], partner).start()

    def chip_max(e):
        remote(own.at[e, 1 - core], pair.at[e], p_send.at[e], p_recv.at[e], partner).wait()
        both[e] = jnp.maximum(own[e, core], pair[e])
        for k in range(1, n // 2):
            remote(both.at[e], chips.at[e, k - 1], z_send.at[e], z_recv.at[e], lax.rem(me + 2 * k, n)).start()

    def all_max(e):
        wait_bytes(chips.at[e], z_send.at[e])
        wait_bytes(chips.at[e], z_recv.at[e])
        top = both[e]
        for k in range(1, n // 2):
            top = jnp.maximum(top, chips[e, k - 1])
        final[e, core] = top
        remote(final.at[e, core], final.at[e, core], f_send.at[e], f_recv.at[e], partner).start()

    def send(e):
        slot = lax.rem(e, 2)

        @pl.when(e + 1 < experts)
        def _():
            for copy in loads(nx, no, nx_sem, no_sem, e + 1):
                copy.start()

        for copy in loads(nx, no, nx_sem, no_sem, e):
            copy.wait()
        remote(final.at[e, core], final.at[e, core], f_send.at[e], f_recv.at[e], partner).wait()
        for t in range(2):
            tops[t, pl.ds(e, 1), :] = final[e, t]
            for j in range(0, columns, LANES):
                latest = nx[slot, t, :, j : j + LANES] + no[slot, t, :, j : j + LANES].astype(jnp.float32)
                turned[j : j + LANES, :] = (latest / final[e, t, :, j : j + LANES]).T

            @pl.when(e >= 2)
            def _():
                wait_bytes(blocks.at[slot, t, pl.ds(0, n - 1)], send_sem.at[slot, t])
                wait_bytes(blocks.at[slot, t, 0], keep_sem.at[slot, t])

            for d in range(n):
                blocks[slot, t, d] = turned[d * width : (d + 1) * width, :].astype(jnp.bfloat16)
            place = outs[t].at[e, :, pl.ds(pl.multiple_of(me * rows, rows), rows)]
            for k in range(n):
                device = lax.rem(me + n // 2 + k, n)
                block = blocks.at[slot, t, device]
                if k == n // 2:
                    pltpu.make_async_copy(block, place, keep_sem.at[slot, t]).start()
                else:
                    remote(block, place, send_sem.at[slot, t], recv_sem.at[t, e], device).start()

    def router_rows():
        pltpu.make_async_copy(part, row.at[me], a_keep).start()
        for k in range(1, n):
            remote(part, row.at[me], a_send, a_recv, lax.rem(me + k, n)).start()

    def router_columns():
        pltpu.make_async_copy(part, row.at[me], a_keep).wait()
        wait_bytes(row.at[pl.ds(0, n - 1)], a_send)
        wait_bytes(row.at[pl.ds(0, n - 1)], a_recv)
        pltpu.make_async_copy(row, whole.at[team], b_keep).start()
        for k in range(1, teams):
            pltpu.make_async_remote_copy(
                src_ref=row, dst_ref=whole.at[team], send_sem=b_send, recv_sem=b_recv,
                device_id={"ep": lax.rem(team + k, teams)}, device_id_type=pl.DeviceIdType.MESH,
            ).start()

    def step(i, carry):
        pl.when(i >= DEPTH)(lambda: send(i - DEPTH))
        pl.when(i < experts)(lambda: measure(i))
        pl.when((i >= 1) & (i < experts + 1))(lambda: chip_max(i - 1))
        pl.when((i >= 2) & (i < experts + 2))(lambda: all_max(i - 2))
        pl.when(i == DEPTH)(router_rows)
        pl.when(i == experts)(router_columns)
        return carry

    lax.fori_loop(0, experts + DEPTH, step, 0)
    for t, out in enumerate((sg, su)):
        for d in range(n):

            @pl.when(me == d)
            def _():
                out[...] = tops[t, :, d * width : (d + 1) * width]

    pltpu.make_async_copy(row, whole.at[team], b_keep).wait()
    wait_bytes(whole.at[pl.ds(0, teams - 1)], b_send)
    wait_bytes(whole.at[pl.ds(0, teams - 1)], b_recv)
    wide, deep = part.shape
    for a in range(teams):
        for d in range(n):
            router[a * wide : (a + 1) * wide, d * deep : (d + 1) * deep] = whole[a, d]
    for slot in range(2):
        for t in range(2):
            wait_bytes(blocks.at[slot, t, pl.ds(0, n - 1)], send_sem.at[slot, t])
            wait_bytes(blocks.at[slot, t, 0], keep_sem.at[slot, t])

    def arrive(e, carry):
        for t in range(2):
            wait_bytes(outs[t].at[e, :, pl.ds(0, (n - 1) * rows)], recv_sem.at[t, e])
        return carry

    lax.fori_loop(0, experts, arrive, 0)


def settle(*refs):
    count = len(refs) // 2
    copies = []
    for src, dst in zip(refs[:count], refs[count:-1]):
        rows = src.shape[0]
        piece = max(rows // PIECES, 1) if len(src.shape) == 3 else rows
        for i in range(0, rows, piece):
            size = min(piece, rows - i)
            copies.append((src.at[pl.ds(i, size)], dst.at[pl.ds(i, size)]))
    copies = [pltpu.make_async_copy(src, dst, refs[-1].at[i]) for i, (src, dst) in enumerate(copies)]
    for copy in copies:
        copy.start()
    for copy in copies:
        copy.wait()


def per_device(n, teams, train_gate, other_gate, train_up, other_up, router_weight, router_gain):
    experts, rows, columns = train_gate.shape
    width = columns // n
    f32, bf16, dma = jnp.float32, jnp.bfloat16, pltpu.SemaphoreType.DMA
    ready = jax.ShapeDtypeStruct((experts, width, rows * n), bf16)
    any_space = pl.BlockSpec(memory_space=pl.ANY)
    part = router_weight.shape[::-1]
    scale = jax.ShapeDtypeStruct((experts, width), f32)
    out_shape = (ready, ready, scale, scale, jax.ShapeDtypeStruct((teams * part[0], n * part[1]), bf16))
    vmem = pl.BlockSpec(memory_space=pltpu.VMEM)
    outs = pl.pallas_call(
        functools.partial(regroup, n, teams),
        out_shape=out_shape,
        in_specs=[any_space] * 4 + [vmem] * 2,
        out_specs=(any_space, any_space, vmem, vmem, vmem),
        scratch_shapes=[
            pltpu.VMEM((2, 2, rows, columns), f32),
            pltpu.VMEM((2, 2, rows, columns), bf16),
            pltpu.VMEM((2, 2, rows, columns), f32),
            pltpu.VMEM((2, 2, rows, columns), bf16),
            pltpu.VMEM((columns, rows), f32),
            pltpu.VMEM((2, 2, n, width, rows), bf16),
            pltpu.VMEM((experts, 2, 1, columns), f32),
            pltpu.VMEM((experts, 1, columns), f32),
            pltpu.VMEM((experts, 1, columns), f32),
            pltpu.VMEM((experts, n // 2 - 1, 1, columns), f32),
            pltpu.VMEM((experts, 2, 1, columns), f32),
            dma((2, 2)),
            dma((2, 2)),
            dma((2, 2)),
            dma((2, 2)),
            dma((2, 2)),
            dma((2, 2)),
            dma((2, experts)),
            dma((experts,)),
            dma((experts,)),
            dma((experts,)),
            dma((experts,)),
            dma((experts,)),
            dma((experts,)),
            pltpu.VMEM((2, experts, columns), f32),
            pltpu.VMEM(part, bf16),
            pltpu.VMEM((n,) + part, bf16),
            pltpu.VMEM((teams, n) + part, bf16),
            dma,
            dma,
            dma,
            dma,
            dma,
            dma,
        ],
        compiler_params=pltpu.CompilerParams(collective_id=0, has_side_effects=True, vmem_limit_bytes=28 * 2**20),
        name="regroup",
    )(train_gate, other_gate, train_up, other_up, router_weight.T, router_gain[None])
    ready_gate, ready_up, scale_gate, scale_up, router = pl.pallas_call(
        settle,
        out_shape=out_shape,
        in_specs=[any_space] * 5,
        out_specs=(any_space,) * 5,
        scratch_shapes=[dma((2 * experts + 3,))],
        compiler_params=pltpu.CompilerParams(vmem_limit_bytes=2**20),
        name="settle",
    )(*outs)
    return jnp.swapaxes(ready_gate, 1, 2), jnp.swapaxes(ready_up, 1, 2), scale_gate, scale_up, router.T


def solution(mesh):
    in_specs = (
        P("ep", "fsdp", None),
        P("ep", "fsdp", None),
        P("ep", "fsdp", None),
        P("ep", "fsdp", None),
        P("fsdp", "ep"),
        P("fsdp"),
    )
    out_specs = (
        P("ep", None, "fsdp"),
        P("ep", None, "fsdp"),
        P("ep", "fsdp"),
        P("ep", "fsdp"),
        P(),
    )
    return jax.shard_map(
        functools.partial(per_device, mesh.shape["fsdp"], mesh.shape["ep"]), mesh=mesh, in_specs=in_specs, out_specs=out_specs,
        check_vma=False,
    )
```

```python
import functools

import jax
import jax.numpy as jnp
from jax import lax
from jax.experimental import pallas as pl
from jax.experimental.pallas import tpu as pltpu
from jax.sharding import PartitionSpec as P

LANES = 128
LAG = 1
PIECES = 8


def regroup(n, teams, tg, og, tu, ou, part, rg, ru, sg, su, router, mx, mo, nx, no, turned, blocks,
            own, pair, both, toright, toleft, fromleft, fromright, chips, zero, mine, theirs, final, tops, row, whole,
            mx_sem, mo_sem, nx_sem, no_sem, send_sem, keep_sem, recv_sem, p_send, p_recv, z_send, z_recv, r_send, r_recv,
            l_send, l_recv, f_send, f_recv, y_send, y_recv, q_send, q_recv, a_send, a_recv, c_send, c_recv, b_send, b_recv):
    me, team = lax.axis_index("fsdp"), lax.axis_index("ep")
    core, chip = lax.rem(me, 2), lax.div(me, 2)
    partner = me + 1 - 2 * core
    line, half = n // 2, n // 2
    last = line - 1
    left = me < half
    far, near = jnp.where(left, half, 0), jnp.where(left, 0, half)
    mirror = lax.rem(me + half, n)
    experts, rows, columns = tg.shape
    width, count = columns // n, columns // LANES
    skipped = columns // 2 // LANES
    shift = jnp.where(left, skipped, 0)
    trains, others, outs = (tg, tu), (og, ou), (rg, ru)
    ahead = [1 + (last - h) * LAG for h in range(line)]
    early = (ahead[0] + 1) // 2

    def measure_loads(e, t):
        slot = lax.rem(e, 2)
        return (
            pltpu.make_async_copy(trains[t].at[e], mx.at[slot, t], mx_sem.at[slot, t]),
            pltpu.make_async_copy(others[t].at[e], mo.at[slot, t], mo_sem.at[slot, t]),
        )

    def send_loads(e, t):
        return (
            pltpu.make_async_copy(trains[t].at[e], nx.at[t], nx_sem.at[t]),
            pltpu.make_async_copy(others[t].at[e], no.at[t], no_sem.at[t]),
        )

    def remote(src, dst, send, recv, device, axis="fsdp"):
        return pltpu.make_async_remote_copy(
            src_ref=src, dst_ref=dst, send_sem=send, recv_sem=recv, device_id={axis: device},
            device_id_type=pl.DeviceIdType.MESH,
        )

    def wait_bytes(ref, sem):
        pltpu.make_async_copy(ref, ref, sem).wait()

    def largest(e, t):
        slot = lax.rem(e, 2)
        for copy in measure_loads(e, t):
            copy.wait()
        for j in range(0, columns, LANES):
            latest = mx[slot, t, :, j : j + LANES] + mo[slot, t, :, j : j + LANES].astype(jnp.float32)
            own[e, t, :, j : j + LANES] = jnp.max(jnp.abs(latest), axis=0, keepdims=True)

    def measure(e):
        @pl.when(e + 1 < experts)
        def _():
            for t in range(2):
                for copy in measure_loads(e + 1, t):
                    copy.start()

        for t in range(2):
            largest(e, t)
        remote(own.at[e, 1 - core], pair.at[e], p_send.at[e], p_recv.at[e], partner).start()

    def chip_max(e):
        remote(own.at[e, 1 - core], pair.at[e], p_send.at[e], p_recv.at[e], partner).wait()
        both[e] = jnp.maximum(own[e, core], pair[e])

    def spread(e):
        for k in range(1, line):
            remote(both.at[e], chips.at[e, k - 1], z_send.at[e], z_recv.at[e], lax.rem(me + 2 * k, n)).start()

    def hop(h, e):
        @pl.when(chip == h)
        def _():
            if h:
                wait_bytes(fromleft.at[e], r_recv.at[e])
                toright[e] = jnp.maximum(both[e], fromleft[e])
            else:
                toright[e] = both[e]
            remote(toright.at[e], fromleft.at[e], r_send.at[e], r_recv.at[e], me + 2).start()

        @pl.when(chip == last - h)
        def _():
            if h:
                wait_bytes(fromright.at[e], l_recv.at[e])
                toleft[e] = jnp.maximum(both[e], fromright[e])
            else:
                toleft[e] = both[e]
            remote(toleft.at[e], fromright.at[e], l_send.at[e], l_recv.at[e], me - 2).start()

    def share(e):
        remote(final.at[e, core], final.at[e, core], f_send.at[e], f_recv.at[e], partner).start()

    def all_direct(e):
        wait_bytes(chips.at[e], z_send.at[e])
        wait_bytes(chips.at[e], z_recv.at[e])
        top = both[e]
        for k in range(1, line):
            top = jnp.maximum(top, chips[e, k - 1])
        final[e, core] = top
        share(e)

    def all_swept(e):
        final[e, core] = both[e]

        @pl.when(chip > 0)
        def _():
            pl.when(chip == last)(lambda: wait_bytes(fromleft.at[e], r_recv.at[e]))
            wait_bytes(toleft.at[e], l_send.at[e])
            final[e, core] = jnp.maximum(final[e, core], fromleft[e])

        @pl.when(chip < last)
        def _():
            pl.when(chip == 0)(lambda: wait_bytes(fromright.at[e], l_recv.at[e]))
            wait_bytes(toright.at[e], r_send.at[e])
            final[e, core] = jnp.maximum(final[e, core], fromright[e])

        share(e)

    def stages(i, s):
        for h in range(line):
            if (ahead[h] + s) % 2:
                continue
            e = i + (ahead[h] + s) // 2
            live = (e >= early) & (e < experts)
            if h == 0:

                @pl.when(live)
                def _():
                    measure(e)
                    chip_max(e)

            if h < last:
                pl.when(live)(lambda: hop(h, e))
            else:
                pl.when(live)(lambda: all_swept(e))
                pl.when(e < early)(lambda: all_direct(e))

    def send(e, t):
        slot = lax.rem(e, 2)
        for copy in send_loads(e, t):
            copy.wait()

        @pl.when(e == 0)
        def _():
            remote(mine.at[t], theirs.at[t], q_send.at[t], q_recv.at[t], partner).wait()
            final[0, t] = jnp.maximum(mine[t], theirs[t])

        if t == 0:

            @pl.when(e > 0)
            def _():
                remote(final.at[e, core], final.at[e, core], f_send.at[e], f_recv.at[e], partner).wait()

        tops[t, pl.ds(e, 1), :] = final[e, t]
        place = outs[t].at[e, :, pl.ds(pl.multiple_of(me * rows, rows), rows)]

        def turn(p):
            j = pl.multiple_of(lax.rem(p + shift, count) * LANES, LANES)
            latest = nx[t, :, pl.ds(j, LANES)] + no[t, :, pl.ds(j, LANES)].astype(jnp.float32)
            turned[pl.ds(j, LANES), :] = (latest / final[e, t, :, pl.ds(j, LANES)]).T

        def pack(base, k):
            d = base + lax.rem(me + k, half)
            blocks[slot, t, d] = turned[pl.ds(pl.multiple_of(d * width, width), width), :].astype(jnp.bfloat16)
            if k == 0:
                pl.when(d == me)(lambda: pltpu.make_async_copy(blocks.at[slot, t, d], place, keep_sem.at[slot, t]).start())
                pl.when(d != me)(lambda: remote(blocks.at[slot, t, d], place, send_sem.at[slot, t], recv_sem.at[t, e], d).start())
            else:
                remote(blocks.at[slot, t, d], place, send_sem.at[slot, t], recv_sem.at[t, e], d).start()

        for p in range(count - skipped):
            turn(p)

        @pl.when(e >= 2)
        def _():
            wait_bytes(blocks.at[slot, t, pl.ds(0, n - 1)], send_sem.at[slot, t])
            wait_bytes(blocks.at[slot, t, 0], keep_sem.at[slot, t])

        for k in range(half):
            pack(far, k)
        for p in range(count - skipped, count):
            turn(p)
        for k in range(half):
            pack(near, k)

        @pl.when(e + 1 < experts)
        def _():
            for copy in send_loads(e + 1, t):
                copy.start()

    def router_cross():
        row[me] = part[...]
        remote(part, row.at[me], a_send, a_recv, mirror).start()

    def router_rows():
        remote(part, row.at[me], a_send, a_recv, mirror).wait()
        for k in range(1, half):
            for at in (me, mirror):
                remote(row.at[at], row.at[at], c_send, c_recv, near + lax.rem(me + k, half)).start()

    def router_columns():
        wait_bytes(row.at[pl.ds(0, 2 * (half - 1))], c_send)
        wait_bytes(row.at[pl.ds(0, 2 * (half - 1))], c_recv)
        whole[team] = row[...]
        for k in range(1, teams):
            remote(row, whole.at[team], b_send, b_recv, lax.rem(team + k, teams), "ep").start()

    def router_whole():
        wait_bytes(whole.at[pl.ds(0, teams - 1)], b_send)
        wait_bytes(whole.at[pl.ds(0, teams - 1)], b_recv)
        wide, deep = part.shape
        for a in range(teams):
            for d in range(n):
                router[a * wide : (a + 1) * wide, d * deep : (d + 1) * deep] = whole[a, d]

    for t in range(2):
        for copy in measure_loads(0, t):
            copy.start()
    barrier = pltpu.get_barrier_semaphore()
    for k in range(1, n):
        pl.semaphore_signal(barrier, inc=1, device_id={"fsdp": lax.rem(me + k, n)}, device_id_type=pl.DeviceIdType.MESH)
    for k in range(1, teams):
        pl.semaphore_signal(barrier, inc=1, device_id={"ep": lax.rem(team + k, teams)}, device_id_type=pl.DeviceIdType.MESH)
    largest(0, 0)
    for t in range(2):
        for copy in measure_loads(1, t):
            copy.start()
    for t in range(2):
        for copy in send_loads(0, t):
            copy.start()
    pl.semaphore_wait(barrier, n + teams - 2)
    for t in range(2):
        if t:
            largest(0, t)
        for k in range(1, line):
            remote(own.at[0, t], zero.at[t, k - 1], y_send.at[t], y_recv.at[t], lax.rem(me + 2 * k, n)).start()
    measure(1)
    for t in range(2):
        wait_bytes(zero.at[t], y_send.at[t])
        wait_bytes(zero.at[t], y_recv.at[t])
        top = own[0, t]
        for k in range(1, line):
            top = jnp.maximum(top, zero[t, k - 1])
        mine[t] = top
        remote(mine.at[t], theirs.at[t], q_send.at[t], q_recv.at[t], partner).start()
    chip_max(1)
    spread(1)

    def early_max(e, carry):
        measure(e)
        chip_max(e)
        spread(e)
        return carry

    def step(i, carry):
        send(i, 0)

        @pl.when(i == 0)
        def _():
            lax.fori_loop(2, early, early_max, 0)

        stages(i, 0)
        send(i, 1)

        stages(i, 1)
        pl.when(i == 1)(router_cross)
        pl.when(i == experts // 4)(router_rows)
        pl.when(i == experts // 2)(router_columns)
        pl.when(i == experts - 2)(router_whole)
        return carry

    lax.fori_loop(0, experts, step, 0)
    for t, out in enumerate((sg, su)):
        for d in range(n):

            @pl.when(me == d)
            def _():
                out[...] = tops[t, :, d * width : (d + 1) * width]

    for slot in range(2):
        for t in range(2):
            wait_bytes(blocks.at[slot, t, pl.ds(0, n - 1)], send_sem.at[slot, t])
            wait_bytes(blocks.at[slot, t, 0], keep_sem.at[slot, t])

    def arrive(e, carry):
        for t in range(2):
            wait_bytes(outs[t].at[e, :, pl.ds(0, (n - 1) * rows)], recv_sem.at[t, e])
        return carry

    lax.fori_loop(0, experts, arrive, 0)


def settle(*refs):
    count = len(refs) // 2
    copies = []
    for src, dst in zip(refs[:count], refs[count:-1]):
        rows = src.shape[0]
        piece = max(rows // PIECES, 1) if len(src.shape) == 3 else rows
        for i in range(0, rows, piece):
            size = min(piece, rows - i)
            copies.append((src.at[pl.ds(i, size)], dst.at[pl.ds(i, size)]))
    copies = [pltpu.make_async_copy(src, dst, refs[-1].at[i]) for i, (src, dst) in enumerate(copies)]
    for copy in copies:
        copy.start()
    for copy in copies:
        copy.wait()


def per_device(n, teams, train_gate, other_gate, train_up, other_up, router_weight, router_gain):
    experts, rows, columns = train_gate.shape
    width = columns // n
    f32, bf16, dma = jnp.float32, jnp.bfloat16, pltpu.SemaphoreType.DMA
    ready = jax.ShapeDtypeStruct((experts, width, rows * n), bf16)
    any_space = pl.BlockSpec(memory_space=pl.ANY)
    part = router_weight.shape[::-1]
    scale = jax.ShapeDtypeStruct((experts, width), f32)
    out_shape = (ready, ready, scale, scale, jax.ShapeDtypeStruct((teams * part[0], n * part[1]), bf16))
    vmem = pl.BlockSpec(memory_space=pltpu.VMEM)
    outs = pl.pallas_call(
        functools.partial(regroup, n, teams),
        out_shape=out_shape,
        in_specs=[any_space] * 4 + [vmem],
        out_specs=(any_space, any_space, vmem, vmem, vmem),
        scratch_shapes=[
            pltpu.VMEM((2, 2, rows, columns), f32),
            pltpu.VMEM((2, 2, rows, columns), bf16),
            pltpu.VMEM((2, rows, columns), f32),
            pltpu.VMEM((2, rows, columns), bf16),
            pltpu.VMEM((columns, rows), f32),
            pltpu.VMEM((2, 2, n, width, rows), bf16),
            pltpu.VMEM((experts, 2, 1, columns), f32),
            *[pltpu.VMEM((experts, 1, columns), f32)] * 6,
            pltpu.VMEM((experts, n // 2 - 1, 1, columns), f32),
            pltpu.VMEM((2, n // 2 - 1, 1, columns), f32),
            pltpu.VMEM((2, 1, columns), f32),
            pltpu.VMEM((2, 1, columns), f32),
            pltpu.VMEM((experts, 2, 1, columns), f32),
            pltpu.VMEM((2, experts, columns), f32),
            pltpu.VMEM((n,) + part, bf16),
            pltpu.VMEM((teams, n) + part, bf16),
            dma((2, 2)),
            dma((2, 2)),
            dma((2,)),
            dma((2,)),
            dma((2, 2)),
            dma((2, 2)),
            dma((2, experts)),
            *[dma((experts,))] * 10,
            *[dma((2,))] * 4,
            *[dma] * 6,
        ],
        compiler_params=pltpu.CompilerParams(collective_id=0, has_side_effects=True, vmem_limit_bytes=28 * 2**20),
        name="regroup",
    )(train_gate, other_gate, train_up, other_up, (router_weight * router_gain[:, None]).astype(bf16).T)
    ready_gate, ready_up, scale_gate, scale_up, router = pl.pallas_call(
        settle,
        out_shape=out_shape,
        in_specs=[any_space] * 5,
        out_specs=(any_space,) * 5,
        scratch_shapes=[dma((2 * experts + 3,))],
        compiler_params=pltpu.CompilerParams(vmem_limit_bytes=2**20),
        name="settle",
    )(*outs)
    return jnp.swapaxes(ready_gate, 1, 2), jnp.swapaxes(ready_up, 1, 2), scale_gate, scale_up, router.T


def solution(mesh):
    in_specs = (
        P("ep", "fsdp", None),
        P("ep", "fsdp", None),
        P("ep", "fsdp", None),
        P("ep", "fsdp", None),
        P("fsdp", "ep"),
        P("fsdp"),
    )
    out_specs = (
        P("ep", None, "fsdp"),
        P("ep", None, "fsdp"),
        P("ep", "fsdp"),
        P("ep", "fsdp"),
        P(),
    )
    return jax.shard_map(
        functools.partial(per_device, mesh.shape["fsdp"], mesh.shape["ep"]), mesh=mesh, in_specs=in_specs, out_specs=out_specs,
        check_vma=False,
    )
```

```python
import functools

import jax
import jax.numpy as jnp
from jax import lax
from jax.experimental import pallas as pl
from jax.experimental.pallas import tpu as pltpu
from jax.sharding import PartitionSpec as P

LANES = 128
LAG = 1
HEAD = 32
PIECES = 8


def regroup(n, teams, tg, og, tu, ou, weight, gain, rg, ru, sg, su, router, mx, mo, nx, no, turned, blocks,
            own, pair, both, toright, toleft, fromleft, fromright, chips, zero, mine, theirs, final, tops, held, gains, part, row, whole, lift, heads, tall, crown,
            mx_sem, mo_sem, nx_sem, no_sem, send_sem, keep_sem, recv_sem, p_send, p_recv, z_send, z_recv, r_send, r_recv,
            l_send, l_recv, f_send, f_recv, y_send, y_recv, q_send, q_recv, a_send, a_recv, c_send, c_recv, b_send, b_recv, g_sem,
            d_send, d_recv, d_keep):
    me, team = lax.axis_index("fsdp"), lax.axis_index("ep")
    core, chip = lax.rem(me, 2), lax.div(me, 2)
    partner = me + 1 - 2 * core
    line, half = n // 2, n // 2
    last = line - 1
    left = me < half
    far, near = jnp.where(left, half, 0), jnp.where(left, 0, half)
    mirror = lax.rem(me + half, n)
    experts, rows, columns = tg.shape
    width, count = columns // n, columns // LANES
    skipped = columns // 2 // LANES
    shift = jnp.where(left, skipped, 0)
    trains, others, outs = (tg, tu), (og, ou), (rg, ru)
    ahead = [1 + (last - h) * LAG for h in range(line)]
    early = (ahead[0] + 1) // 2
    head = heads.shape[1]
    rest = pl.ds(head, width - head)

    def measure_loads(e, t):
        slot = lax.rem(e, 2)
        return (
            pltpu.make_async_copy(trains[t].at[e], mx.at[slot, t], mx_sem.at[slot, t]),
            pltpu.make_async_copy(others[t].at[e], mo.at[slot, t], mo_sem.at[slot, t]),
        )

    def send_loads(e, t):
        return (
            pltpu.make_async_copy(trains[t].at[e], nx.at[t], nx_sem.at[t]),
            pltpu.make_async_copy(others[t].at[e], no.at[t], no_sem.at[t]),
        )

    def remote(src, dst, send, recv, device, axis="fsdp"):
        return pltpu.make_async_remote_copy(
            src_ref=src, dst_ref=dst, send_sem=send, recv_sem=recv, device_id={axis: device},
            device_id_type=pl.DeviceIdType.MESH,
        )

    def wait_bytes(ref, sem):
        pltpu.make_async_copy(ref, ref, sem).wait()

    def largest(e, t):
        slot = lax.rem(e, 2)
        for copy in measure_loads(e, t):
            copy.wait()
        for j in range(0, columns, LANES):
            latest = mx[slot, t, :, j : j + LANES] + mo[slot, t, :, j : j + LANES].astype(jnp.float32)
            own[e, t, :, j : j + LANES] = jnp.max(jnp.abs(latest), axis=0, keepdims=True)

    def zero_send(t):
        for k in range(1, line):
            remote(own.at[0, t], zero.at[t, k - 1], y_send.at[t], y_recv.at[t], lax.rem(me + 2 * k, n)).start()

    def zero_max(t):
        wait_bytes(zero.at[t], y_send.at[t])
        wait_bytes(zero.at[t], y_recv.at[t])
        top = own[0, t]
        for k in range(1, line):
            top = jnp.maximum(top, zero[t, k - 1])
        mine[t] = top
        remote(mine.at[t], theirs.at[t], q_send.at[t], q_recv.at[t], partner).start()

    def head_turn(p):
        j = pl.multiple_of(lax.rem(p + shift, count) * LANES, LANES)
        latest = mx[0, 0, :, pl.ds(j, LANES)] + mo[0, 0, :, pl.ds(j, LANES)].astype(jnp.float32)
        lift[pl.ds(j, LANES), :] = latest.T

    def head_send(base, first):
        for k in range(first, half):
            d = base + lax.rem(me + k, half)
            remote(lift.at[pl.ds(pl.multiple_of(d * width, width), head)], heads.at[me], d_send, d_recv, d).start()

    def head_settle():
        wait_bytes(heads.at[pl.ds(0, n - 1)], d_send)
        wait_bytes(heads.at[pl.ds(0, n - 1)], d_recv)
        for j in range(0, columns, LANES):
            tall[j : j + LANES, :] = jnp.broadcast_to(final[0, 0, :, j : j + LANES], (LANES, LANES)).T
        scale = tall[pl.ds(pl.multiple_of(me * width, width), head), 0:1]
        for d in range(n):
            crown[:, d * rows : (d + 1) * rows] = (heads[d] / scale).astype(jnp.bfloat16)
        pltpu.make_async_copy(crown, rg.at[0, pl.ds(0, head)], d_keep).start()

    def measure(e):
        @pl.when(e + 1 < experts)
        def _():
            for t in range(2):
                for copy in measure_loads(e + 1, t):
                    copy.start()

        for t in range(2):
            largest(e, t)
        remote(own.at[e, 1 - core], pair.at[e], p_send.at[e], p_recv.at[e], partner).start()

    def chip_max(e):
        remote(own.at[e, 1 - core], pair.at[e], p_send.at[e], p_recv.at[e], partner).wait()
        both[e] = jnp.maximum(own[e, core], pair[e])

    def spread(e):
        for k in range(1, line):
            remote(both.at[e], chips.at[e, k - 1], z_send.at[e], z_recv.at[e], lax.rem(me + 2 * k, n)).start()

    def hop(h, e):
        @pl.when(chip == h)
        def _():
            if h:
                wait_bytes(fromleft.at[e], r_recv.at[e])
                toright[e] = jnp.maximum(both[e], fromleft[e])
            else:
                toright[e] = both[e]
            remote(toright.at[e], fromleft.at[e], r_send.at[e], r_recv.at[e], me + 2).start()

        @pl.when(chip == last - h)
        def _():
            if h:
                wait_bytes(fromright.at[e], l_recv.at[e])
                toleft[e] = jnp.maximum(both[e], fromright[e])
            else:
                toleft[e] = both[e]
            remote(toleft.at[e], fromright.at[e], l_send.at[e], l_recv.at[e], me - 2).start()

    def share(e):
        remote(final.at[e, core], final.at[e, core], f_send.at[e], f_recv.at[e], partner).start()

    def all_direct(e):
        wait_bytes(chips.at[e], z_send.at[e])
        wait_bytes(chips.at[e], z_recv.at[e])
        top = both[e]
        for k in range(1, line):
            top = jnp.maximum(top, chips[e, k - 1])
        final[e, core] = top
        share(e)

    def all_swept(e):
        final[e, core] = both[e]

        @pl.when(chip > 0)
        def _():
            pl.when(chip == last)(lambda: wait_bytes(fromleft.at[e], r_recv.at[e]))
            wait_bytes(toleft.at[e], l_send.at[e])
            final[e, core] = jnp.maximum(final[e, core], fromleft[e])

        @pl.when(chip < last)
        def _():
            pl.when(chip == 0)(lambda: wait_bytes(fromright.at[e], l_recv.at[e]))
            wait_bytes(toright.at[e], r_send.at[e])
            final[e, core] = jnp.maximum(final[e, core], fromright[e])

        share(e)

    def stages(i, s):
        for h in range(line):
            if (ahead[h] + s) % 2:
                continue
            e = i + (ahead[h] + s) // 2
            live = (e >= early) & (e < experts)
            if h == 0:

                @pl.when(live)
                def _():
                    measure(e)
                    chip_max(e)

            if h < last:
                pl.when(live)(lambda: hop(h, e))
            else:
                pl.when(live)(lambda: all_swept(e))
                pl.when(e < early)(lambda: all_direct(e))

    def send(e, t):
        slot = lax.rem(e, 2)
        for copy in send_loads(e, t):
            copy.wait()

        @pl.when(e == 0)
        def _():
            remote(mine.at[t], theirs.at[t], q_send.at[t], q_recv.at[t], partner).wait()
            final[0, t] = jnp.maximum(mine[t], theirs[t])

        if t == 0:

            @pl.when(e > 0)
            def _():
                remote(final.at[e, core], final.at[e, core], f_send.at[e], f_recv.at[e], partner).wait()

        tops[t, pl.ds(e, 1), :] = final[e, t]
        place = outs[t].at[e, :, pl.ds(pl.multiple_of(me * rows, rows), rows)]

        def turn(p):
            j = pl.multiple_of(lax.rem(p + shift, count) * LANES, LANES)
            latest = nx[t, :, pl.ds(j, LANES)] + no[t, :, pl.ds(j, LANES)].astype(jnp.float32)
            turned[pl.ds(j, LANES), :] = (latest / final[e, t, :, pl.ds(j, LANES)]).T

        def pack(base, k, here=False):
            d = base + lax.rem(me + k, half)
            blocks[slot, t, d] = turned[pl.ds(pl.multiple_of(d * width, width), width), :].astype(jnp.bfloat16)
            block = blocks.at[slot, t, d]

            def go(src, dst):
                if here:
                    pltpu.make_async_copy(src, dst, keep_sem.at[slot, t]).start()
                else:
                    remote(src, dst, send_sem.at[slot, t], recv_sem.at[t, e], d).start()

            if t == 0:
                pl.when(e == 0)(lambda: go(block.at[rest], place.at[rest]))
                pl.when(e > 0)(lambda: go(block, place))
            else:
                go(block, place)

        for p in range(count - skipped):
            turn(p)

        @pl.when(e >= (2 if t else 3))
        def _():
            wait_bytes(blocks.at[slot, t, pl.ds(0, n - 1)], send_sem.at[slot, t])
            wait_bytes(blocks.at[slot, t, 0], keep_sem.at[slot, t])

        if t == 0:

            @pl.when(e == 2)
            def _():
                wait_bytes(blocks.at[0, 0, pl.ds(0, n - 1), rest], send_sem.at[0, 0])
                wait_bytes(blocks.at[0, 0, 0, rest], keep_sem.at[0, 0])

        for k in range(half):
            pack(far, k)
        for p in range(count - skipped, count):
            turn(p)
        for k in range(half):
            pack(near, k, k == 0)

        @pl.when(e + 1 < experts)
        def _():
            for copy in send_loads(e + 1, t):
                copy.start()

    def router_cross():
        for copy in router_loads:
            copy.wait()
        part[...] = (held[...] * gains[...]).astype(jnp.bfloat16)
        row[me] = part[...]
        remote(part, row.at[me], a_send, a_recv, mirror).start()

    def router_rows():
        remote(part, row.at[me], a_send, a_recv, mirror).wait()
        for k in range(1, half):
            for at in (me, mirror):
                remote(row.at[at], row.at[at], c_send, c_recv, near + lax.rem(me + k, half)).start()

    def router_columns():
        wait_bytes(row.at[pl.ds(0, 2 * (half - 1))], c_send)
        wait_bytes(row.at[pl.ds(0, 2 * (half - 1))], c_recv)
        whole[team] = row[...]
        for k in range(1, teams):
            remote(row, whole.at[team], b_send, b_recv, lax.rem(team + k, teams), "ep").start()

    def router_whole():
        wait_bytes(whole.at[pl.ds(0, teams - 1)], b_send)
        wait_bytes(whole.at[pl.ds(0, teams - 1)], b_recv)
        wide, deep = part.shape
        for a in range(teams):
            for d in range(n):
                router[a * wide : (a + 1) * wide, d * deep : (d + 1) * deep] = whole[a, d]

    for copy in measure_loads(0, 0):
        copy.start()
    barrier = pltpu.get_barrier_semaphore()
    for k in range(1, n):
        pl.semaphore_signal(barrier, inc=1, device_id={"fsdp": lax.rem(me + k, n)}, device_id_type=pl.DeviceIdType.MESH)
    for k in range(1, teams):
        pl.semaphore_signal(barrier, inc=1, device_id={"ep": lax.rem(team + k, teams)}, device_id_type=pl.DeviceIdType.MESH)
    router_loads = (pltpu.make_async_copy(weight, held, g_sem.at[0]), pltpu.make_async_copy(gain, gains, g_sem.at[1]))
    loads = [*measure_loads(0, 1), *measure_loads(1, 0), *measure_loads(1, 1), *send_loads(0, 0), *send_loads(0, 1), *router_loads]
    for copy in loads:
        copy.start()
    largest(0, 0)
    for p in range(count - skipped):
        head_turn(p)
    pl.semaphore_wait(barrier, n + teams - 2)
    zero_send(0)
    head_send(far, 0)
    largest(0, 1)
    zero_send(1)
    for p in range(count - skipped, count):
        head_turn(p)
    head_send(near, 1)
    heads[me] = lift[pl.ds(pl.multiple_of(me * width, width), head), :]
    measure(1)
    chip_max(1)
    spread(1)
    zero_max(0)

    def early_max(e, carry):
        measure(e)
        chip_max(e)
        spread(e)
        return carry

    def step(i, carry):
        send(i, 0)

        @pl.when(i == 0)
        def _():
            zero_max(1)
            lax.fori_loop(2, early, early_max, 0)

        stages(i, 0)
        send(i, 1)

        stages(i, 1)
        pl.when(i == 1)(router_cross)
        pl.when(i == 2)(head_settle)
        pl.when(i == experts // 4)(router_rows)
        pl.when(i == experts // 2)(router_columns)
        pl.when(i == experts - 2)(router_whole)
        return carry

    lax.fori_loop(0, experts, step, 0)
    for t, out in enumerate((sg, su)):
        for d in range(n):

            @pl.when(me == d)
            def _():
                out[...] = tops[t, :, d * width : (d + 1) * width]

    for slot in range(2):
        for t in range(2):
            wait_bytes(blocks.at[slot, t, pl.ds(0, n - 1)], send_sem.at[slot, t])
            wait_bytes(blocks.at[slot, t, 0], keep_sem.at[slot, t])

    def arrive(e, carry):
        for t in range(2):
            wait_bytes(outs[t].at[e, :, pl.ds(0, (n - 1) * rows)], recv_sem.at[t, e])
        return carry

    wait_bytes(rg.at[0, rest, pl.ds(0, (n - 1) * rows)], recv_sem.at[0, 0])
    wait_bytes(ru.at[0, :, pl.ds(0, (n - 1) * rows)], recv_sem.at[1, 0])
    lax.fori_loop(1, experts, arrive, 0)
    pltpu.make_async_copy(crown, rg.at[0, pl.ds(0, head)], d_keep).wait()


def settle(*refs):
    count = len(refs) // 2
    copies = []
    for src, dst in zip(refs[:count], refs[count:-1]):
        rows = src.shape[0]
        piece = max(rows // PIECES, 1) if len(src.shape) == 3 else rows
        for i in range(0, rows, piece):
            size = min(piece, rows - i)
            copies.append((src.at[pl.ds(i, size)], dst.at[pl.ds(i, size)]))
    copies = [pltpu.make_async_copy(src, dst, refs[-1].at[i]) for i, (src, dst) in enumerate(copies)]
    for copy in copies:
        copy.start()
    for copy in copies:
        copy.wait()


def per_device(n, teams, train_gate, other_gate, train_up, other_up, router_weight, router_gain):
    experts, rows, columns = train_gate.shape
    width = columns // n
    f32, bf16, dma = jnp.float32, jnp.bfloat16, pltpu.SemaphoreType.DMA
    ready = jax.ShapeDtypeStruct((experts, width, rows * n), bf16)
    any_space = pl.BlockSpec(memory_space=pl.ANY)
    head = min(HEAD, width // 2)
    part = router_weight.shape[::-1]
    in_hbm = functools.partial(pltpu.with_memory_space_constraint, memory_space=pltpu.HBM)
    scale = jax.ShapeDtypeStruct((experts, width), f32)
    out_shape = (ready, ready, scale, scale, jax.ShapeDtypeStruct((teams * part[0], n * part[1]), bf16))
    vmem = pl.BlockSpec(memory_space=pltpu.VMEM)
    outs = pl.pallas_call(
        functools.partial(regroup, n, teams),
        out_shape=out_shape,
        in_specs=[any_space] * 6,
        out_specs=(any_space, any_space, vmem, vmem, vmem),
        scratch_shapes=[
            pltpu.VMEM((2, 2, rows, columns), f32),
            pltpu.VMEM((2, 2, rows, columns), bf16),
            pltpu.VMEM((2, rows, columns), f32),
            pltpu.VMEM((2, rows, columns), bf16),
            pltpu.VMEM((columns, rows), f32),
            pltpu.VMEM((2, 2, n, width, rows), bf16),
            pltpu.VMEM((experts, 2, 1, columns), f32),
            *[pltpu.VMEM((experts, 1, columns), f32)] * 6,
            pltpu.VMEM((experts, n // 2 - 1, 1, columns), f32),
            pltpu.VMEM((2, n // 2 - 1, 1, columns), f32),
            pltpu.VMEM((2, 1, columns), f32),
            pltpu.VMEM((2, 1, columns), f32),
            pltpu.VMEM((experts, 2, 1, columns), f32),
            pltpu.VMEM((2, experts, columns), f32),
            pltpu.VMEM(part, f32),
            pltpu.VMEM((1, part[1]), f32),
            pltpu.VMEM(part, bf16),
            pltpu.VMEM((n,) + part, bf16),
            pltpu.VMEM((teams, n) + part, bf16),
            pltpu.VMEM((columns, rows), f32),
            pltpu.VMEM((n, head, rows), f32),
            pltpu.VMEM((columns, LANES), f32),
            pltpu.VMEM((head, rows * n), bf16),
            dma((2, 2)),
            dma((2, 2)),
            dma((2,)),
            dma((2,)),
            dma((2, 2)),
            dma((2, 2)),
            dma((2, experts)),
            *[dma((experts,))] * 10,
            *[dma((2,))] * 4,
            *[dma] * 6,
            dma((2,)),
            *[dma] * 3,
        ],
        compiler_params=pltpu.CompilerParams(collective_id=0, has_side_effects=True, vmem_limit_bytes=28 * 2**20),
        name="regroup",
    )(train_gate, other_gate, train_up, other_up, in_hbm(router_weight.T), in_hbm(router_gain[None]))
    ready_gate, ready_up, scale_gate, scale_up, router = pl.pallas_call(
        settle,
        out_shape=out_shape,
        in_specs=[any_space] * 5,
        out_specs=(any_space,) * 5,
        scratch_shapes=[dma((2 * experts + 3,))],
        compiler_params=pltpu.CompilerParams(vmem_limit_bytes=2**20),
        name="settle",
    )(*outs)
    return jnp.swapaxes(ready_gate, 1, 2), jnp.swapaxes(ready_up, 1, 2), scale_gate, scale_up, router.T


def solution(mesh):
    in_specs = (
        P("ep", "fsdp", None),
        P("ep", "fsdp", None),
        P("ep", "fsdp", None),
        P("ep", "fsdp", None),
        P("fsdp", "ep"),
        P("fsdp"),
    )
    out_specs = (
        P("ep", None, "fsdp"),
        P("ep", None, "fsdp"),
        P("ep", "fsdp"),
        P("ep", "fsdp"),
        P(),
    )
    return jax.shard_map(
        functools.partial(per_device, mesh.shape["fsdp"], mesh.shape["ep"]), mesh=mesh, in_specs=in_specs, out_specs=out_specs,
        check_vma=False,
    )
```
